32 devices in a mesh: row: 4 (over z), col: 8 (over y, x, core).
Axes of the slice: x: 2, y: 2, z: 4, core: 2. Of those that a mesh axis runs over, the one named last changes fastest.
Arguments:
- features: bfloat16 [64, 131072], P(None, ('row', 'col')), may hold values from -6 to 6
- tile_rows: int32 [4, 8, 512], P('row', 'col'), may hold values from 0 to 255, as said below
- tile_cols: int32 [4, 8, 512], P('row', 'col'), may hold values from 0 to 127
- tile_count: int32 [4, 8], P('row', 'col'), may hold values from 1 to 512, as said below
- tile_data: bfloat16 [4, 8, 512, 128, 128], P('row', 'col'), may hold values from -0.21875 to 0.21875
Outputs:
- filtered: bfloat16 [512, 131072], P(None, ('row', 'col'))
The draws below stay inside these ranges and needn't reach their ends.
Inputs may be any that keep to these rules, and one draw needn't show every extreme that they name: Within one device the pairs (tile_rows, tile_cols) of all 512 slots are distinct. `tile_count`: some device has all 512 slots live in every draw.
All inputs are finite; a program needn't handle non-finite values.
Results may differ from the reference program's by a relative error of at most 0.009.
Values may be sent and summed in bfloat16 or wider, within the bound.
A program may use at most 128 MiB of HBM per device.

```python
import jax
import jax.numpy as jnp
from jax import lax

CHANNELS = 64
SCALES = 8
TILE_SIZE = 128
NODES_DEV = 4096
TILES_MAX = 512
NODES = 131072
BLOCK_ROWS = 256
N_ROW = 4
N_COL = 8


def tile_cells(key):
    row_blocks = NODES_DEV * N_COL // TILE_SIZE
    col_blocks = NODES_DEV * N_ROW // TILE_SIZE
    keys = jax.random.split(jax.random.fold_in(key, 11), N_ROW * N_COL)

    def one_device(device_key):
        return jax.random.permutation(device_key, row_blocks * col_blocks)[:TILES_MAX]
    cells = jax.vmap(one_device)(keys)
    return (cells.reshape(N_ROW, N_COL, TILES_MAX).astype(jnp.int32), col_blocks)


def draw_tile_rows(key, part):
    cells, col_blocks = tile_cells(key)
    return (cells // col_blocks).astype(jnp.int32)


def draw_tile_cols(key, part):
    cells, col_blocks = tile_cells(key)
    return (cells % col_blocks).astype(jnp.int32)


def draw_tile_count(key, part):
    device_count = N_ROW * N_COL
    base_key = jax.random.fold_in(key, 23)
    full_key = jax.random.fold_in(key, 29)
    lowest = max(1, TILES_MAX // 8)
    highest = max(lowest + 1, TILES_MAX // 2 + 1)
    counts = jax.random.randint(base_key, (device_count,), lowest, highest).astype(jnp.int32)
    chosen = jax.random.permutation(full_key, device_count)[:max(1, device_count // 16)]
    counts = counts.at[chosen].set(TILES_MAX)
    return counts.reshape(N_ROW, N_COL).astype(jnp.int32)


def levels(key, shape, pieces, least, top_value):
    loudness, own = 1.0, jax.random.fold_in(key, 6)
    for axis_at, shards_of in pieces:
        draws = jnp.exp(jax.random.uniform(jax.random.fold_in(own, axis_at), (shards_of,), jnp.float32, least / len(pieces), top_value / len(pieces)))
        loudness = loudness * jnp.repeat(draws, shape[axis_at] // shards_of).reshape([-1 if axis == axis_at else 1 for axis in range(len(shape))])
    return loudness


def centred(stream_key, shape, deviation, bound, shards=(), kind=jnp.bfloat16):
    array = jax.random.normal(stream_key, shape, jnp.float32) * deviation
    if len(shards) > 0:
        array = levels(stream_key, shape, shards, -0.22, 0.18) * array
    return jnp.clip(array, min=-bound, max=bound).astype(kind)


def setup_inputs(seed: int = 0) -> dict:
    arg_keys = jax.random.split(jax.random.key(seed), 6)
    return {
        "features": centred(arg_keys[0], (CHANNELS, NODES), 1.0, 6.0, ((1, 32),)),
        "tile_rows": draw_tile_rows(jax.random.fold_in(arg_keys[5], 71), 0),
        "tile_cols": draw_tile_cols(jax.random.fold_in(arg_keys[5], 71), 0),
        "tile_count": draw_tile_count(jax.random.fold_in(arg_keys[5], 71), 0),
        "tile_data": centred(arg_keys[4], (N_ROW, N_COL, TILES_MAX, TILE_SIZE, TILE_SIZE), 768 ** -0.5, 0.21875, ((0, 4), (1, 8))),
    }


def bessel_pair(times):
    halved = times / 2.0
    square = halved * halved
    term_zero = jnp.ones_like(times)
    term_one = halved
    sum_zero = term_zero
    sum_one = term_one
    for degree in range(1, 24):
        term_zero = term_zero * square / float(degree * degree)
        term_one = term_one * square / float(degree * (degree + 1))
        sum_zero = sum_zero + term_zero
        sum_one = sum_one + term_one
    damping = jnp.exp(-times)
    return damping * sum_zero, damping * sum_one


def coefficients():
    times = 0.25 * 2.0 ** (jnp.arange(SCALES).astype(jnp.float32) / 2.0)
    bessel_zero, bessel_one = bessel_pair(times)
    return bessel_zero, -2.0 * bessel_one, 2.0 * (bessel_zero - 2.0 * bessel_one / times)


def apply_operator(field, tile_rows, tile_cols, tile_count, tile_data):
    per_block = NODES_DEV // TILE_SIZE
    blocks = field.reshape(CHANNELS, NODES // TILE_SIZE, TILE_SIZE)
    device_count = N_ROW * N_COL
    slot_rows = tile_rows.reshape(device_count, TILES_MAX)
    slot_cols = tile_cols.reshape(device_count, TILES_MAX)
    slot_live = tile_count.reshape(device_count)
    slot_data = tile_data.reshape(device_count, TILES_MAX, TILE_SIZE, TILE_SIZE)

    def one_device(summed, inputs):
        row_ids, col_ids, live_count, entries, device = inputs
        row_group = device // N_COL
        col_group = device % N_COL
        global_cols = ((col_ids // per_block) * N_COL + col_group) * per_block + col_ids % per_block
        picked = jnp.take(blocks, global_cols.astype(jnp.int32), axis=1)
        product = jnp.einsum("fgk,grk->fgr", picked.astype(jnp.float32), entries.astype(jnp.float32))
        live = (jnp.arange(TILES_MAX) < live_count).astype(jnp.float32)
        product = product * live[None, :, None]
        partial_value = jnp.zeros((CHANNELS, BLOCK_ROWS, TILE_SIZE), jnp.float32).at[:, row_ids].add(product)
        partial_value = partial_value.astype(jnp.bfloat16).astype(jnp.float32)
        offset = (row_group * BLOCK_ROWS).astype(jnp.int32)
        current = lax.dynamic_slice_in_dim(summed, offset, BLOCK_ROWS, 1)
        summed = lax.dynamic_update_slice_in_dim(summed, current + partial_value, offset, 1)
        return summed, None

    start = jnp.zeros((CHANNELS, NODES // TILE_SIZE, TILE_SIZE), jnp.float32)
    device_ids = jnp.arange(device_count).astype(jnp.int32)
    summed, _ = lax.scan(one_device, start, (slot_rows, slot_cols, slot_live, slot_data, device_ids))
    return summed.reshape(CHANNELS, NODES).astype(jnp.bfloat16)


def reference(features, tile_rows, tile_cols, tile_count, tile_data):
    first = apply_operator(features, tile_rows, tile_cols, tile_count, tile_data)
    second = apply_operator(first, tile_rows, tile_cols, tile_count, tile_data)
    coef_zero, coef_one, coef_two = coefficients()
    base = features.astype(jnp.float32)
    first_wide = first.astype(jnp.float32)
    second_wide = second.astype(jnp.float32)
    filtered = (coef_zero[:, None, None] * base[None] + coef_one[:, None, None] * first_wide[None]
                + coef_two[:, None, None] * (2.0 * second_wide - base)[None])
    return filtered.reshape(SCALES * CHANNELS, NODES).astype(jnp.bfloat16)
```

```python
import functools

import jax
import jax.numpy as jnp
import numpy as np
from jax import lax
from jax.experimental import pallas as pl
from jax.experimental.pallas import tpu as pltpu
from jax.sharding import PartitionSpec as P

SCALES = 8
TILE = 128
MESH = pl.DeviceIdType.MESH
VMEM = pltpu.VMEM
CHUNKS = (16, 16, 16, 16)
UNROLL = 64
PIECES = 8
REACH = 2


def coefficients():
    times = np.float32(0.25) * np.float32(2.0) ** (np.arange(SCALES).astype(np.float32) / np.float32(2.0))
    halved = times / np.float32(2.0)
    square = halved * halved
    term_zero = np.ones_like(times)
    term_one = halved
    sum_zero, sum_one = term_zero, term_one
    for degree in range(1, 24):
        term_zero = term_zero * square / np.float32(degree * degree)
        term_one = term_one * square / np.float32(degree * (degree + 1))
        sum_zero = sum_zero + term_zero
        sum_one = sum_one + term_one
    damping = np.exp(-times)
    zero, one = damping * sum_zero, damping * sum_one
    return zero, np.float32(-2.0) * one, np.float32(2.0) * (zero - np.float32(2.0) * one / times)


def sign_of(way):
    return 1 - 2 * way


def body(plan, meta_ref, keep_ref, last_ref, features_ref, data_ref, first_ref, second_ref, *scratch):
    row_size, col_size, slots, slot_bits, col_bits = plan
    chunks = len(CHUNKS)
    phases = 2 * chunks
    names = list(scratch)
    panels = [names.pop(0) for _ in range(phases)]
    arrived_a = [names.pop(0) for _ in range(phases)]
    arrived_b = [names.pop(0) for _ in range(phases)]
    partials = [names.pop(0) for _ in range(2)]
    tiles, sums, field, own_sem, tile_sem, zsend, zrecv, asend, arecv, bsend, brecv = names
    width = [CHUNKS[p % chunks] for p in range(phases)]
    start = [sum(CHUNKS[: p % chunks]) for p in range(phases)]
    chips = col_size // 2
    per_block = first_ref.shape[1] // TILE
    row_blocks = col_size * per_block

    me = lax.axis_index("row")
    col = lax.axis_index("col")
    side = lax.rem(col, 2)
    chip = col // 2

    def own_copy(p):
        rows = pl.ds(start[p], width[p])
        return pltpu.make_async_copy(features_ref.at[rows], field.at[rows], own_sem.at[p])

    def tile_copy(piece):
        part = pl.ds(piece * (slots // PIECES), slots // PIECES)
        return pltpu.make_async_copy(data_ref.at[part], tiles.at[part], tile_sem.at[piece])

    for p in range(chunks):
        own_copy(p).start()
    for piece in range(PIECES):
        tile_copy(piece).start()

    barrier = pltpu.get_barrier_semaphore()
    expected = jnp.int32(0)
    for sign in (1, -1):
        for hop in range(1, min(REACH, row_size - 1) + 1):
            peer = me + sign * hop
            inside = jnp.logical_and(peer >= 0, peer < row_size)
            expected = expected + inside.astype(jnp.int32)

            @pl.when(inside)
            def _():
                pl.semaphore_signal(barrier, inc=1, device_id={"row": peer}, device_id_type=MESH)

    pl.semaphore_signal(barrier, inc=1, device_id={"col": col + 1 - 2 * side}, device_id_type=MESH)
    for step in range(1, chips):
        peer = 2 * lax.rem(chip + step, chips) + side
        pl.semaphore_signal(barrier, inc=1, device_id={"col": peer}, device_id_type=MESH)
    pl.semaphore_wait(barrier, expected + chips)

    def zcopy(p, way, hop):
        sign = sign_of(way)
        relayed = hop > REACH
        origin = me - sign * (hop - 1) if relayed else me
        target = me + sign if relayed else me + sign * hop
        inside = jnp.logical_and(target >= 0, target < row_size)
        if relayed:
            inside = jnp.logical_and(inside, jnp.logical_and(origin >= 0, origin < row_size))
        block = panels[p].at[pl.ds(origin * per_block, per_block)]
        copy = pltpu.make_async_remote_copy(
            src_ref=block,
            dst_ref=block,
            send_sem=zsend.at[p, way, hop - 1],
            recv_sem=zrecv.at[p, way, hop - 1],
            device_id={"row": target},
            device_id_type=MESH,
        )
        return inside, copy

    def zarrival(p, way, hop):
        sign = sign_of(way)
        origin = me - sign * hop
        inside = jnp.logical_and(origin >= 0, origin < row_size)
        block = panels[p].at[pl.ds(origin * per_block, per_block)]
        copy = pltpu.make_async_remote_copy(
            src_ref=block,
            dst_ref=block,
            send_sem=zsend.at[p, way, hop - 1],
            recv_sem=zrecv.at[p, way, hop - 1],
            device_id={"row": origin},
            device_id_type=MESH,
        )
        return inside, copy

    def send_own(p):
        for hop in range(min(REACH, row_size - 1), 0, -1):
            for way in range(2):
                inside, copy = zcopy(p, way, hop)
                pl.when(inside)(copy.start)

    def relay(p):
        for hop in range(REACH + 1, row_size):
            for way in range(2):
                inside, copy = zcopy(p, way, hop)
                landed = zarrival(p, way, hop - 1)[1]

                @pl.when(inside)
                def _():
                    landed.wait_recv()
                    copy.start()

    def receive(p):
        for hop in range(1, row_size):
            for way in range(2):
                inside, landed = zarrival(p, way, hop)
                if REACH <= hop < row_size - 1:
                    onward = me + sign_of(way)
                    passes = jnp.logical_and(onward >= 0, onward < row_size)
                    inside = jnp.logical_and(inside, jnp.logical_not(passes))
                pl.when(inside)(landed.wait_recv)

    def products(p, low, high, carry):
        lanes_mask = (1 << col_bits) - 1
        channels = width[p]

        def group(index, total):
            left, right = [], []
            for offset in range(UNROLL):
                word = meta_ref[index * UNROLL + offset]
                column = jnp.bitwise_and(lax.shift_right_logical(word, slot_bits), lanes_mask)
                left.append(panels[p][column])
                right.append(tiles[jnp.bitwise_and(word, slots - 1)])
            parts = []
            for at in range(0, UNROLL, 2):
                both = jnp.dot(
                    jnp.concatenate(left[at : at + 2], 0),
                    jnp.concatenate(right[at : at + 2], 1),
                    preferred_element_type=jnp.float32,
                )
                parts += [both[:channels, :TILE], both[channels:, TILE:]]
            for offset in range(UNROLL):
                total = total * keep_ref[index * UNROLL + offset] + parts[offset]
                sums[1 + index * UNROLL + offset] = total
            return total

        return lax.fori_loop(low, high, group, carry)

    def finish(p):
        channels = width[p]

        def rows(step, carry):
            for offset in range(8):
                at = step * 8 + offset
                dest = at // per_block
                partials[p % 2][lax.rem(dest, 2), dest // 2, lax.rem(at, per_block)] = sums[
                    last_ref[at]
                ].astype(jnp.bfloat16)
            return carry

        lax.fori_loop(0, row_blocks // 8, rows, 0)

    def acopy(p):
        return pltpu.make_async_remote_copy(
            src_ref=partials[p % 2].at[1 - side],
            dst_ref=arrived_a[p],
            send_sem=asend.at[p],
            recv_sem=arecv.at[p],
            device_id={"col": col + 1 - 2 * side},
            device_id_type=MESH,
        )

    def bcopy(p, step):
        target = lax.rem(chip + step, chips)
        return pltpu.make_async_remote_copy(
            src_ref=partials[p % 2].at[side, target],
            dst_ref=arrived_b[p].at[step - 1],
            send_sem=bsend.at[p, step - 1],
            recv_sem=brecv.at[p, step - 1],
            device_id={"col": 2 * target + side},
            device_id_type=MESH,
        )

    def pair_sum(p):
        acopy(p).wait_recv()
        for step in [*range(1, chips), 0]:
            target = lax.rem(chip + step, chips)
            total = partials[p % 2][side, target].astype(jnp.float32) + arrived_a[p][target].astype(jnp.float32)
            partials[p % 2][side, target] = total.astype(jnp.bfloat16)
            if step:
                bcopy(p, step).start()

    def chip_sum(p):
        total = partials[p % 2][side, chip].astype(jnp.float32)
        for step in range(1, chips):
            bcopy(p, step).wait_recv()
            total = total + arrived_b[p][step - 1].astype(jnp.float32)
        result = total.astype(jnp.bfloat16)
        if p < chunks:
            panels[p + chunks][pl.ds(me * per_block, per_block)] = result
            send_own(p + chunks)
        out_ref = first_ref if p < chunks else second_ref
        for block in range(per_block):
            out_ref[start[p] : start[p] + width[p], block * TILE : (block + 1) * TILE] = result[block]

    def settle(p):
        acopy(p).wait_send()
        for step in range(1, chips):
            bcopy(p, step).wait_send()

    for p in range(chunks):
        own_copy(p).wait()
        for block in range(per_block):
            panels[p][me * per_block + block] = field[
                start[p] : start[p] + width[p], block * TILE : (block + 1) * TILE
            ]
        if p < 2:
            send_own(p)

    for piece in range(PIECES):
        tile_copy(piece).wait()

        def turn(step, carry):
            for offset in range(4):
                at = piece * (slots // PIECES) + step * 4 + offset
                tiles[at] = tiles[at].T
            return carry

        lax.fori_loop(0, slots // PIECES // 4, turn, 0)

    sums[0] = jnp.zeros(sums.shape[1:], jnp.float32)

    groups = slots // UNROLL
    relay(0)
    for p in range(phases):
        receive(p)
        carry = jnp.zeros((width[p], TILE), jnp.float32)
        carry = products(p, 0, groups // 2, carry)
        if p >= 1:
            chip_sum(p - 1)
        carry = products(p, groups // 2, groups, carry)
        if p >= 2:
            settle(p - 2)
        finish(p)
        acopy(p).start()
        pair_sum(p)
        if p + 1 < phases:
            relay(p + 1)
        if p + 2 < chunks:
            send_own(p + 2)
    chip_sum(phases - 1)

    for p in (phases - 2, phases - 1):
        settle(p)
    for p in range(phases):
        for way in range(2):
            for hop in range(1, row_size):
                inside, copy = zcopy(p, way, hop)
                pl.when(inside)(copy.wait_send)


def slot_order(slot_rows, slot_cols, live_count, row_blocks, slot_bits, col_bits):
    slots = slot_rows.shape[0]
    index = jnp.arange(slots, dtype=jnp.int32)
    row = jnp.where(index < live_count, slot_rows, row_blocks)
    key = row * slots + index
    rank = jnp.sum((key[None, :] < key[:, None]).astype(jnp.int32), axis=1)
    word = index + (slot_cols << slot_bits) + (row << (slot_bits + col_bits))
    sorted_words = jnp.sum(jnp.where(rank[:, None] == index[None, :], word[:, None], 0), axis=0)
    before = lax.shift_right_logical(jnp.roll(sorted_words, 1), slot_bits + col_bits)
    same = before == lax.shift_right_logical(sorted_words, slot_bits + col_bits)
    keep = jnp.where(jnp.logical_and(same, index > 0), 1.0, 0.0)
    blocks = jnp.arange(row_blocks, dtype=jnp.int32)
    until = jnp.sum((row[:, None] <= blocks[None, :]).astype(jnp.int32), axis=0)
    before = jnp.sum((row[:, None] < blocks[None, :]).astype(jnp.int32), axis=0)
    return sorted_words, keep, jnp.where(until == before, 0, until)


def shards(features, tile_rows, tile_cols, tile_count, tile_data):
    row_size, col_size = lax.axis_size("row"), lax.axis_size("col")
    channels, nodes = features.shape
    slot_rows = tile_rows.reshape(-1)
    slot_cols = tile_cols.reshape(-1)
    slot_data = tile_data.reshape(-1, TILE, TILE)
    slots = slot_rows.shape[0]
    row_blocks = col_size * nodes // TILE
    slot_bits = (slots - 1).bit_length()
    col_bits = (row_size * nodes // TILE - 1).bit_length()
    words, keep, last = slot_order(
        slot_rows, slot_cols, tile_count.reshape(()), row_blocks, slot_bits, col_bits
    )
    phases = 2 * len(CHUNKS)
    chips = col_size // 2
    widths = [CHUNKS[p % len(CHUNKS)] for p in range(phases)]
    field = jax.ShapeDtypeStruct((channels, nodes), jnp.bfloat16)
    dma = pltpu.SemaphoreType.DMA
    wide = max(CHUNKS)
    per_block = nodes // TILE
    scratch = [VMEM((row_size * per_block, w, TILE), jnp.bfloat16) for w in widths]
    scratch += [VMEM((chips, per_block, w, TILE), jnp.bfloat16) for w in widths]
    scratch += [VMEM((chips - 1, per_block, w, TILE), jnp.bfloat16) for w in widths]
    scratch += [VMEM((2, chips, per_block, wide, TILE), jnp.bfloat16)] * 2
    scratch += [
        VMEM((slots, TILE, TILE), jnp.bfloat16),
        VMEM((slots + 1, wide, TILE), jnp.float32),
        VMEM((channels, nodes), jnp.bfloat16),
        dma((len(CHUNKS),)),
        dma((PIECES,)),
        dma((phases, 2, row_size - 1)),
        dma((phases, 2, row_size - 1)),
        dma((phases,)),
        dma((phases,)),
        dma((phases, chips - 1)),
        dma((phases, chips - 1)),
    ]
    first, second = pl.pallas_call(
        functools.partial(body, (row_size, col_size, slots, slot_bits, col_bits)),
        out_shape=(field, field),
        in_specs=[
            pl.BlockSpec(memory_space=pltpu.SMEM),
            pl.BlockSpec(memory_space=pltpu.SMEM),
            pl.BlockSpec(memory_space=pltpu.SMEM),
            pl.BlockSpec(memory_space=pl.ANY),
            pl.BlockSpec(memory_space=pl.ANY),
        ],
        out_specs=(pl.BlockSpec(memory_space=VMEM), pl.BlockSpec(memory_space=VMEM)),
        scratch_shapes=scratch,
        compiler_params=pltpu.CompilerParams(
            collective_id=0, has_side_effects=True, vmem_limit_bytes=60 * 2**20
        ),
        name="operator_twice",
    )(words, keep, last, features, slot_data)

    coef_zero, coef_one, coef_two = coefficients()
    base = features.astype(jnp.float32)
    first_wide = first.astype(jnp.float32)
    second_wide = second.astype(jnp.float32)
    filtered = (
        coef_zero[:, None, None] * base[None]
        + coef_one[:, None, None] * first_wide[None]
        + coef_two[:, None, None] * (2.0 * second_wide - base)[None]
    )
    return filtered.reshape(-1, nodes).astype(jnp.bfloat16)


def solution(mesh):
    return jax.shard_map(
        shards,
        mesh=mesh,
        in_specs=(
            P(None, ("row", "col")),
            P("row", "col", None),
            P("row", "col", None),
            P("row", "col"),
            P("row", "col", None, None, None),
        ),
        out_specs=P(None, ("row", "col")),
        check_vma=False,
    )
```

```python
import functools

import jax
import jax.numpy as jnp
import numpy as np
from jax import lax
from jax.experimental import pallas as pl
from jax.experimental.pallas import tpu as pltpu
from jax.sharding import PartitionSpec as P

SCALES = 8
TILE = 128
MESH = pl.DeviceIdType.MESH
VMEM = pltpu.VMEM
CHUNKS = (16, 16, 16, 16)
UNROLL = TILE
PIECES = 8
REACH = 2
AHEAD = 3


def coefficients():
    times = np.float32(0.25) * np.float32(2.0) ** (np.arange(SCALES).astype(np.float32) / np.float32(2.0))
    halved = times / np.float32(2.0)
    square = halved * halved
    term_zero = np.ones_like(times)
    term_one = halved
    sum_zero, sum_one = term_zero, term_one
    for degree in range(1, 24):
        term_zero = term_zero * square / np.float32(degree * degree)
        term_one = term_one * square / np.float32(degree * (degree + 1))
        sum_zero = sum_zero + term_zero
        sum_one = sum_one + term_one
    damping = np.exp(-times)
    zero, one = damping * sum_zero, damping * sum_one
    return zero, np.float32(-2.0) * one, np.float32(2.0) * (zero - np.float32(2.0) * one / times)


def sign_of(way):
    return 1 - 2 * way


def body(plan, rows_ref, cols_ref, count_ref, features_ref, data_ref, first_ref, second_ref, *scratch):
    row_size, col_size, slots, slot_bits, col_bits = plan
    chunks = len(CHUNKS)
    phases = 2 * chunks
    names = list(scratch)
    panels = [names.pop(0) for _ in range(phases)]
    arrived_a = [names.pop(0) for _ in range(phases)]
    arrived_b = [names.pop(0) for _ in range(phases)]
    partials = [names.pop(0) for _ in range(2)]
    tiles, sums, field, words, keeps, lasts, meta_ref, keep_ref, last_ref, order_sem, own_sem, tile_sem, zsend, zrecv, asend, arecv, bsend, brecv = names
    width = [CHUNKS[p % chunks] for p in range(phases)]
    start = [sum(CHUNKS[: p % chunks]) for p in range(phases)]
    chips = col_size // 2
    per_block = first_ref.shape[1] // TILE
    row_blocks = col_size * per_block

    me = lax.axis_index("row")
    col = lax.axis_index("col")
    side = lax.rem(col, 2)
    chip = col // 2

    def own_copy(p):
        rows = pl.ds(start[p], width[p])
        return pltpu.make_async_copy(features_ref.at[rows], field.at[rows], own_sem.at[p])

    def tile_copy(piece):
        part = pl.ds(piece * (slots // PIECES), slots // PIECES)
        return pltpu.make_async_copy(data_ref.at[part], tiles.at[part], tile_sem.at[piece])

    for p in range(chunks):
        own_copy(p).start()
    for piece in range(PIECES):
        tile_copy(piece).start()

    barrier = pltpu.get_barrier_semaphore()
    expected = jnp.int32(0)
    for sign in (1, -1):
        for hop in range(1, min(REACH, row_size - 1) + 1):
            peer = me + sign * hop
            inside = jnp.logical_and(peer >= 0, peer < row_size)
            expected = expected + inside.astype(jnp.int32)

            @pl.when(inside)
            def _():
                pl.semaphore_signal(barrier, inc=1, device_id={"row": peer}, device_id_type=MESH)

    pl.semaphore_signal(barrier, inc=1, device_id={"col": col + 1 - 2 * side}, device_id_type=MESH)
    for step in range(1, chips):
        peer = 2 * lax.rem(chip + step, chips) + side
        pl.semaphore_signal(barrier, inc=1, device_id={"col": peer}, device_id_type=MESH)
    pl.semaphore_wait(barrier, expected + chips)

    def within(at):
        return jnp.logical_and(at >= 0, at < row_size)

    def last_of(way):
        return row_size - 1 if way == 0 else 0

    def zcopy(p, way, hop, origin, target, place=0):
        block = panels[p].at[pl.ds(origin * per_block, per_block)]
        return pltpu.make_async_remote_copy(
            src_ref=block,
            dst_ref=block,
            send_sem=zsend.at[p, way, place + hop - 1],
            recv_sem=zrecv.at[p, way, hop - 1],
            device_id={"row": target},
            device_id_type=MESH,
        )

    def direct(p, way, hop):
        target = me + sign_of(way) * hop
        inside = within(target)
        if hop > 1:
            inside = jnp.logical_and(inside, target != last_of(way))
        return inside, zcopy(p, way, hop, me, target)

    def relayed(p, way, hop):
        target = me + sign_of(way)
        origin = target - sign_of(way) * hop
        inside = jnp.logical_and(within(target), within(origin))
        if hop <= REACH:
            inside = jnp.logical_and(inside, target == last_of(way))
        return inside, zcopy(p, way, hop, origin, target, row_size)

    def landed(p, way, hop):
        origin = me - sign_of(way) * hop
        return within(origin), zcopy(p, way, hop, origin, origin)

    direct_hops = range(min(REACH, row_size - 1), 0, -1)
    relay_hops = range(2, row_size)

    def send_own(p):
        for hop in direct_hops:
            for way in range(2):
                inside, copy = direct(p, way, hop)
                pl.when(inside)(copy.start)

    def relay(p):
        for hop in relay_hops:
            for way in range(2):
                inside, copy = relayed(p, way, hop)
                arrival = landed(p, way, hop - 1)[1]

                @pl.when(inside)
                def _():
                    arrival.wait_recv()
                    copy.start()

    def receive(p):
        for hop in range(1, row_size):
            for way in range(2):
                inside, arrival = landed(p, way, hop)
                target = me + sign_of(way)
                passes = within(target)
                if hop + 1 <= REACH:
                    passes = jnp.logical_and(passes, target == last_of(way))
                inside = jnp.logical_and(inside, jnp.logical_not(passes))
                pl.when(inside)(arrival.wait_recv)

    def sent(p):
        for way in range(2):
            for hop in direct_hops:
                inside, copy = direct(p, way, hop)
                pl.when(inside)(copy.wait_send)
            for hop in relay_hops:
                inside, copy = relayed(p, way, hop)
                pl.when(inside)(copy.wait_send)

    def products(p):
        lanes_mask = (1 << col_bits) - 1
        channels = width[p]

        def group(index, total):
            left, right = [], []
            for offset in range(UNROLL):
                word = meta_ref[index, offset]
                column = jnp.bitwise_and(lax.shift_right_logical(word, slot_bits), lanes_mask)
                left.append(panels[p][column])
                right.append(tiles[jnp.bitwise_and(word, slots - 1)])
            parts = []
            for at in range(0, UNROLL, 2):
                both = jnp.dot(
                    jnp.concatenate(left[at : at + 2], 0),
                    jnp.concatenate(right[at : at + 2], 1),
                    preferred_element_type=jnp.float32,
                )
                parts += [both[:channels, :TILE], both[channels:, TILE:]]
            for offset in range(UNROLL):
                total = total * keep_ref[index, offset] + parts[offset]
                sums[1 + index * UNROLL + offset] = total
            return total

        empty = jnp.zeros((channels, TILE), jnp.float32)
        lax.fori_loop(0, slots // UNROLL, group, empty)

    def finish(p):
        def rows(dest, carry):
            chip_of, side_of = dest // 2, lax.rem(dest, 2)
            line, first_at = dest * per_block // TILE, lax.rem(dest * per_block, TILE)
            for block in range(per_block):
                partials[p % 2][side_of, chip_of, block] = sums[
                    last_ref[line, first_at + block]
                ].astype(jnp.bfloat16)
            return carry

        lax.fori_loop(0, col_size, rows, 0)

    def acopy(p):
        return pltpu.make_async_remote_copy(
            src_ref=partials[p % 2].at[1 - side],
            dst_ref=arrived_a[p],
            send_sem=asend.at[p],
            recv_sem=arecv.at[p],
            device_id={"col": col + 1 - 2 * side},
            device_id_type=MESH,
        )

    def bcopy(p, step):
        target = lax.rem(chip + step, chips)
        return pltpu.make_async_remote_copy(
            src_ref=partials[p % 2].at[side, target],
            dst_ref=arrived_b[p].at[step - 1],
            send_sem=bsend.at[p, step - 1],
            recv_sem=brecv.at[p, step - 1],
            device_id={"col": 2 * target + side},
            device_id_type=MESH,
        )

    def pair_sum(p):
        acopy(p).wait_recv()
        for step in [*range(1, chips), 0]:
            target = lax.rem(chip + step, chips)
            total = partials[p % 2][side, target].astype(jnp.float32) + arrived_a[p][target].astype(jnp.float32)
            partials[p % 2][side, target] = total.astype(jnp.bfloat16)
            if step:
                bcopy(p, step).start()

    def chip_sum(p):
        total = partials[p % 2][side, chip].astype(jnp.float32)
        for step in range(1, chips):
            bcopy(p, step).wait_recv()
            total = total + arrived_b[p][step - 1].astype(jnp.float32)
        result = total.astype(jnp.bfloat16)
        if p < chunks:
            panels[p + chunks][pl.ds(me * per_block, per_block)] = result
            send_own(p + chunks)
        out_ref = first_ref if p < chunks else second_ref
        for block in range(per_block):
            out_ref[start[p] : start[p] + width[p], block * TILE : (block + 1) * TILE] = result[block]

    def settle(p):
        acopy(p).wait_send()
        for step in range(1, chips):
            bcopy(p, step).wait_send()

    for p in range(chunks):
        own_copy(p).wait()
        for block in range(per_block):
            panels[p][me * per_block + block] = field[
                start[p] : start[p] + width[p], block * TILE : (block + 1) * TILE
            ]
        if p < AHEAD:
            send_own(p)

    def order():
        live = count_ref[0, 0]
        square = (TILE, TILE)
        lane = lax.broadcasted_iota(jnp.int32, square, 1)
        none = jnp.zeros(square, jnp.int32)
        keys, rows_lane, keys_down, rows_down, words_down = [], [], [], [], []
        pieces = slots // TILE
        for piece in range(pieces):
            part = slice(piece * TILE, (piece + 1) * TILE)
            index = lane + piece * TILE
            row = jnp.where(index < live, jnp.broadcast_to(rows_ref[0, :, part], square), row_blocks)
            word = index + jnp.broadcast_to(cols_ref[0, :, part], square) * slots
            keys.append(row * slots + index)
            rows_lane.append(row)
            keys_down.append(keys[-1].T)
            rows_down.append(row.T)
            words_down.append(word.T)
        ranks, repeats = [], []
        for piece in range(pieces):
            ahead, same = none, none
            for other in range(pieces):
                less = jnp.where(keys_down[other] < keys[piece], 1, 0)
                ahead = ahead + less
                same = same + jnp.where(rows_down[other] == rows_lane[piece], less, 0)
            ahead = jnp.sum(ahead, axis=0, keepdims=True)
            same = jnp.minimum(jnp.sum(same, axis=0, keepdims=True), 1)
            ranks.append(jnp.broadcast_to(ahead, square).T)
            repeats.append(jnp.broadcast_to(same, square).T)
        for piece in range(pieces):
            place = lane + piece * TILE
            word, keep = none, none
            for other in range(pieces):
                here = ranks[other] == place
                word = word + jnp.where(here, words_down[other], 0)
                keep = keep + jnp.where(here, repeats[other], 0)
            words[piece : piece + 1] = jnp.sum(word, axis=0, keepdims=True)
            keeps[piece : piece + 1] = jnp.sum(keep, axis=0, keepdims=True).astype(jnp.float32)
        for piece in range(row_blocks // TILE):
            place = lane + piece * TILE
            until, before = none, none
            for other in range(pieces):
                until = until + jnp.where(rows_down[other] <= place, 1, 0)
                before = before + jnp.where(rows_down[other] < place, 1, 0)
            until = jnp.sum(until, axis=0, keepdims=True)
            before = jnp.sum(before, axis=0, keepdims=True)
            lasts[piece : piece + 1] = jnp.where(until == before, 0, until)
        moves = [
            pltpu.make_async_copy(source, target, order_sem.at[at])
            for at, (source, target) in enumerate(((words, meta_ref), (keeps, keep_ref), (lasts, last_ref)))
        ]
        for move in moves:
            move.start()
        for move in moves:
            move.wait()

    order()

    for piece in range(PIECES):
        tile_copy(piece).wait()

        def turn(step, carry):
            for offset in range(4):
                at = piece * (slots // PIECES) + step * 4 + offset
                tiles[at] = tiles[at].T
            return carry

        lax.fori_loop(0, slots // PIECES // 4, turn, 0)
        if piece == PIECES // 2:
            relay(0)
            if chunks > AHEAD:
                send_own(AHEAD)

    sums[0] = jnp.zeros(sums.shape[1:], jnp.float32)

    for p in range(phases):
        receive(p)
        if p + 1 < phases:
            relay(p + 1)
        if p + 1 + AHEAD < chunks:
            send_own(p + 1 + AHEAD)
        products(p)
        if p >= 2:
            settle(p - 2)
        finish(p)
        acopy(p).start()
        pair_sum(p)
        if p >= 1:
            chip_sum(p - 1)
    chip_sum(phases - 1)

    for p in (phases - 2, phases - 1):
        settle(p)
    for p in range(phases):
        sent(p)


def filter_bank(coefs, base_ref, first_ref, second_ref, out_ref):
    base = base_ref[...].astype(jnp.float32)
    first = first_ref[...].astype(jnp.float32)
    rest = 2.0 * second_ref[...].astype(jnp.float32) - base
    for scale, (zero, one, two) in enumerate(coefs):
        out_ref[scale] = (zero * base + one * first + two * rest).astype(out_ref.dtype)


def shards(features, tile_rows, tile_cols, tile_count, tile_data):
    row_size, col_size = lax.axis_size("row"), lax.axis_size("col")
    channels, nodes = features.shape
    slots = tile_rows.shape[2]
    slot_data = tile_data.reshape(slots, TILE, TILE)
    row_blocks = col_size * nodes // TILE
    slot_bits = (slots - 1).bit_length()
    col_bits = (row_size * nodes // TILE - 1).bit_length()
    phases = 2 * len(CHUNKS)
    chips = col_size // 2
    widths = [CHUNKS[p % len(CHUNKS)] for p in range(phases)]
    field = jax.ShapeDtypeStruct((channels, nodes), jnp.bfloat16)
    dma = pltpu.SemaphoreType.DMA
    wide = max(CHUNKS)
    per_block = nodes // TILE
    scratch = [VMEM((row_size * per_block, w, TILE), jnp.bfloat16) for w in widths]
    scratch += [VMEM((chips, per_block, w, TILE), jnp.bfloat16) for w in widths]
    scratch += [VMEM((chips - 1, per_block, w, TILE), jnp.bfloat16) for w in widths]
    scratch += [VMEM((2, chips, per_block, wide, TILE), jnp.bfloat16)] * 2
    scratch += [
        VMEM((slots, TILE, TILE), jnp.bfloat16),
        VMEM((slots + 1, wide, TILE), jnp.float32),
        VMEM((channels, nodes), jnp.bfloat16),
        VMEM((slots // TILE, TILE), jnp.int32),
        VMEM((slots // TILE, TILE), jnp.float32),
        VMEM((row_blocks // TILE, TILE), jnp.int32),
        pltpu.SMEM((slots // TILE, TILE), jnp.int32),
        pltpu.SMEM((slots // TILE, TILE), jnp.float32),
        pltpu.SMEM((row_blocks // TILE, TILE), jnp.int32),
        dma((3,)),
        dma((len(CHUNKS),)),
        dma((PIECES,)),
        dma((phases, 2, 2 * row_size)),
        dma((phases, 2, row_size)),
        dma((phases,)),
        dma((phases,)),
        dma((phases, chips - 1)),
        dma((phases, chips - 1)),
    ]
    first, second = pl.pallas_call(
        functools.partial(body, (row_size, col_size, slots, slot_bits, col_bits)),
        out_shape=(field, field),
        in_specs=[
            pl.BlockSpec(memory_space=VMEM),
            pl.BlockSpec(memory_space=VMEM),
            pl.BlockSpec(memory_space=pltpu.SMEM),
            pl.BlockSpec(memory_space=pl.ANY),
            pl.BlockSpec(memory_space=pl.ANY),
        ],
        out_specs=(pl.BlockSpec(memory_space=VMEM), pl.BlockSpec(memory_space=VMEM)),
        scratch_shapes=scratch,
        compiler_params=pltpu.CompilerParams(
            collective_id=0, has_side_effects=True, vmem_limit_bytes=60 * 2**20
        ),
        name="operator_twice",
    )(tile_rows, tile_cols, tile_count, features, slot_data)

    depth = 16
    coefs = [tuple(float(c) for c in row) for row in zip(*coefficients())]
    rows = pl.BlockSpec((depth, nodes), lambda i: (i, 0))
    filtered = pl.pallas_call(
        functools.partial(filter_bank, coefs),
        out_shape=jax.ShapeDtypeStruct((SCALES, channels, nodes), jnp.bfloat16),
        grid=(channels // depth,),
        in_specs=[rows, rows, rows],
        out_specs=pl.BlockSpec((SCALES, depth, nodes), lambda i: (0, i, 0)),
        name="filter_bank",
    )(features, first, second)
    return filtered.reshape(SCALES * channels, nodes)


def solution(mesh):
    return jax.shard_map(
        shards,
        mesh=mesh,
        in_specs=(
            P(None, ("row", "col")),
            P("row", "col", None),
            P("row", "col", None),
            P("row", "col"),
            P("row", "col", None, None, None),
        ),
        out_specs=P(None, ("row", "col")),
        check_vma=False,
    )
```

```python
import functools

import jax
import jax.numpy as jnp
import numpy as np
from jax import lax
from jax.experimental import pallas as pl
from jax.experimental.pallas import tpu as pltpu
from jax.sharding import PartitionSpec as P

SCALES = 8
TILE = 128
MESH = pl.DeviceIdType.MESH
VMEM = pltpu.VMEM
CHUNKS = (16, 16, 16, 16)
UNROLL = TILE
PIECES = 8
REACH = 2
AHEAD = 4


def coefficients():
    times = np.float32(0.25) * np.float32(2.0) ** (np.arange(SCALES).astype(np.float32) / np.float32(2.0))
    halved = times / np.float32(2.0)
    square = halved * halved
    term_zero = np.ones_like(times)
    term_one = halved
    sum_zero, sum_one = term_zero, term_one
    for degree in range(1, 24):
        term_zero = term_zero * square / np.float32(degree * degree)
        term_one = term_one * square / np.float32(degree * (degree + 1))
        sum_zero = sum_zero + term_zero
        sum_one = sum_one + term_one
    damping = np.exp(-times)
    zero, one = damping * sum_zero, damping * sum_one
    return zero, np.float32(-2.0) * one, np.float32(2.0) * (zero - np.float32(2.0) * one / times)


def sign_of(way):
    return 1 - 2 * way


def body(plan, rows_ref, cols_ref, count_ref, features_ref, data_ref, first_ref, second_ref, *scratch):
    row_size, col_size, slots, slot_bits, col_bits = plan
    chunks = len(CHUNKS)
    phases = 2 * chunks
    names = list(scratch)
    panels = [names.pop(0) for _ in range(phases)]
    arrived_a = [names.pop(0) for _ in range(phases)]
    arrived_b = [names.pop(0) for _ in range(phases)]
    kinds = sorted(set(CHUNKS))
    by_kind = {w: (names.pop(0), names.pop(0), names.pop(0)) for w in kinds}
    tiles, field, words, keeps, lasts, meta_ref, keep_ref, last_ref, order_sem, own_sem, tile_sem, zsend, zrecv, asend, arecv, bsend, brecv = names
    width = [CHUNKS[p % chunks] for p in range(phases)]
    start = [sum(CHUNKS[: p % chunks]) for p in range(phases)]
    partials = [by_kind[width[p]][p % 2] for p in range(phases)]
    sums = [by_kind[width[p]][2] for p in range(phases)]
    chips = col_size // 2
    per_block = first_ref.shape[1] // TILE
    row_blocks = col_size * per_block

    me = lax.axis_index("row")
    col = lax.axis_index("col")
    side = lax.rem(col, 2)
    chip = col // 2

    def own_copy(p):
        rows = pl.ds(start[p], width[p])
        return pltpu.make_async_copy(features_ref.at[rows], field.at[rows], own_sem.at[p])

    def tile_copy(piece):
        part = pl.ds(piece * (slots // PIECES), slots // PIECES)
        return pltpu.make_async_copy(data_ref.at[part], tiles.at[part], tile_sem.at[piece])

    for p in range(chunks):
        own_copy(p).start()
    for piece in range(PIECES):
        tile_copy(piece).start()

    barrier = pltpu.get_barrier_semaphore()
    expected = jnp.int32(0)
    for sign in (1, -1):
        for hop in range(1, min(REACH, row_size - 1) + 1):
            peer = me + sign * hop
            inside = jnp.logical_and(peer >= 0, peer < row_size)
            expected = expected + inside.astype(jnp.int32)

            @pl.when(inside)
            def _():
                pl.semaphore_signal(barrier, inc=1, device_id={"row": peer}, device_id_type=MESH)

    pl.semaphore_signal(barrier, inc=1, device_id={"col": col + 1 - 2 * side}, device_id_type=MESH)
    for step in range(1, chips):
        peer = 2 * lax.rem(chip + step, chips) + side
        pl.semaphore_signal(barrier, inc=1, device_id={"col": peer}, device_id_type=MESH)
    pl.semaphore_wait(barrier, expected + chips)

    def within(at):
        return jnp.logical_and(at >= 0, at < row_size)

    def last_of(way):
        return row_size - 1 if way == 0 else 0

    def zcopy(p, way, hop, origin, target, place=0):
        block = panels[p].at[pl.ds(origin * per_block, per_block)]
        return pltpu.make_async_remote_copy(
            src_ref=block,
            dst_ref=block,
            send_sem=zsend.at[p, way, place + hop - 1],
            recv_sem=zrecv.at[p, way, hop - 1],
            device_id={"row": target},
            device_id_type=MESH,
        )

    def direct(p, way, hop):
        target = me + sign_of(way) * hop
        inside = within(target)
        if hop > 1:
            inside = jnp.logical_and(inside, target != last_of(way))
        return inside, zcopy(p, way, hop, me, target)

    def relayed(p, way, hop):
        target = me + sign_of(way)
        origin = target - sign_of(way) * hop
        inside = jnp.logical_and(within(target), within(origin))
        if hop <= REACH:
            inside = jnp.logical_and(inside, target == last_of(way))
        return inside, zcopy(p, way, hop, origin, target, row_size)

    def landed(p, way, hop):
        origin = me - sign_of(way) * hop
        return within(origin), zcopy(p, way, hop, origin, origin)

    direct_hops = range(min(REACH, row_size - 1), 0, -1)
    relay_hops = range(2, row_size)

    def send_own(p):
        for hop in direct_hops:
            for way in range(2):
                inside, copy = direct(p, way, hop)
                pl.when(inside)(copy.start)

    def relay(p):
        for hop in relay_hops:
            for way in range(2):
                inside, copy = relayed(p, way, hop)
                arrival = landed(p, way, hop - 1)[1]

                @pl.when(inside)
                def _():
                    arrival.wait_recv()
                    copy.start()

    def receive(p):
        for hop in range(1, row_size):
            for way in range(2):
                inside, arrival = landed(p, way, hop)
                target = me + sign_of(way)
                passes = within(target)
                if hop + 1 <= REACH:
                    passes = jnp.logical_and(passes, target == last_of(way))
                inside = jnp.logical_and(inside, jnp.logical_not(passes))
                pl.when(inside)(arrival.wait_recv)

    def sent(p):
        for way in range(2):
            for hop in direct_hops:
                inside, copy = direct(p, way, hop)
                pl.when(inside)(copy.wait_send)
            for hop in relay_hops:
                inside, copy = relayed(p, way, hop)
                pl.when(inside)(copy.wait_send)

    def products(p):
        lanes_mask = (1 << col_bits) - 1
        channels = width[p]

        def group(index, total):
            left, right = [], []
            for offset in range(UNROLL):
                word = meta_ref[index, offset]
                column = jnp.bitwise_and(lax.shift_right_logical(word, slot_bits), lanes_mask)
                left.append(panels[p][column])
                right.append(tiles[jnp.bitwise_and(word, slots - 1)])
            parts = []
            for at in range(0, UNROLL, 2):
                both = jnp.dot(
                    jnp.concatenate(left[at : at + 2], 0),
                    jnp.concatenate(right[at : at + 2], 1),
                    preferred_element_type=jnp.float32,
                )
                parts += [both[:channels, :TILE], both[channels:, TILE:]]
            for offset in range(UNROLL):
                total = total * keep_ref[index, offset] + parts[offset]
                sums[p][1 + index * UNROLL + offset] = total
            return total

        empty = jnp.zeros((channels, TILE), jnp.float32)
        lax.fori_loop(0, slots // UNROLL, group, empty)

    def finish(p):
        def rows(target, side_of):
            dest = 2 * target + side_of
            line, first_at = dest * per_block // TILE, lax.rem(dest * per_block, TILE)
            for block in range(per_block):
                partials[p][side_of, target, block] = sums[p][
                    last_ref[line, first_at + block]
                ].astype(jnp.bfloat16)

        def given(step, carry):
            target = lax.rem(chip + step, chips)
            rows(target, 1 - side)
            acopy(p, target).start()
            return carry

        def kept(target, carry):
            rows(target, side)
            return carry

        lax.fori_loop(1, chips + 1, given, 0)
        lax.fori_loop(0, chips, kept, 0)

    def acopy(p, target):
        return pltpu.make_async_remote_copy(
            src_ref=partials[p].at[1 - side, target],
            dst_ref=arrived_a[p].at[target],
            send_sem=asend.at[p, target],
            recv_sem=arecv.at[p, target],
            device_id={"col": col + 1 - 2 * side},
            device_id_type=MESH,
        )

    def bcopy(p, step):
        target = lax.rem(chip + step, chips)
        return pltpu.make_async_remote_copy(
            src_ref=partials[p].at[side, target],
            dst_ref=arrived_b[p].at[step - 1],
            send_sem=bsend.at[p, step - 1],
            recv_sem=brecv.at[p, step - 1],
            device_id={"col": 2 * target + side},
            device_id_type=MESH,
        )

    def pair_sum(p):
        for step in [*range(1, chips), 0]:
            target = lax.rem(chip + step, chips)
            acopy(p, target).wait_recv()
            total = partials[p][side, target].astype(jnp.float32) + arrived_a[p][target].astype(jnp.float32)
            partials[p][side, target] = total.astype(jnp.bfloat16)
            if step:
                bcopy(p, step).start()

    def chip_sum(p):
        total = partials[p][side, chip].astype(jnp.float32)
        for step in range(1, chips):
            bcopy(p, step).wait_recv()
            total = total + arrived_b[p][step - 1].astype(jnp.float32)
        result = total.astype(jnp.bfloat16)
        if p < chunks:
            panels[p + chunks][pl.ds(me * per_block, per_block)] = result
            send_own(p + chunks)
        out_ref = first_ref if p < chunks else second_ref
        for block in range(per_block):
            out_ref[start[p] : start[p] + width[p], block * TILE : (block + 1) * TILE] = result[block]

    def settle(p):
        for target in range(chips):
            acopy(p, target).wait_send()
        for step in range(1, chips):
            bcopy(p, step).wait_send()

    for p in range(chunks):
        own_copy(p).wait()
        for block in range(per_block):
            panels[p][me * per_block + block] = field[
                start[p] : start[p] + width[p], block * TILE : (block + 1) * TILE
            ]
        if p < AHEAD:
            send_own(p)

    def order():
        live = count_ref[0, 0]
        square = (TILE, TILE)
        lane = lax.broadcasted_iota(jnp.int32, square, 1)
        none = jnp.zeros(square, jnp.int32)
        keys, rows_lane, keys_down, rows_down, words_down = [], [], [], [], []
        pieces = slots // TILE
        for piece in range(pieces):
            part = slice(piece * TILE, (piece + 1) * TILE)
            index = lane + piece * TILE
            row = jnp.where(index < live, jnp.broadcast_to(rows_ref[0, :, part], square), row_blocks)
            word = index + jnp.broadcast_to(cols_ref[0, :, part], square) * slots
            keys.append(row * slots + index)
            rows_lane.append(row)
            keys_down.append(keys[-1].T)
            rows_down.append(row.T)
            words_down.append(word.T)
        ranks, repeats = [], []
        for piece in range(pieces):
            ahead, same = none, none
            for other in range(pieces):
                less = jnp.where(keys_down[other] < keys[piece], 1, 0)
                ahead = ahead + less
                same = same + jnp.where(rows_down[other] == rows_lane[piece], less, 0)
            ahead = jnp.sum(ahead, axis=0, keepdims=True)
            same = jnp.minimum(jnp.sum(same, axis=0, keepdims=True), 1)
            ranks.append(jnp.broadcast_to(ahead, square).T)
            repeats.append(jnp.broadcast_to(same, square).T)
        for piece in range(pieces):
            place = lane + piece * TILE
            word, keep = none, none
            for other in range(pieces):
                here = ranks[other] == place
                word = word + jnp.where(here, words_down[other], 0)
                keep = keep + jnp.where(here, repeats[other], 0)
            words[piece : piece + 1] = jnp.sum(word, axis=0, keepdims=True)
            keeps[piece : piece + 1] = jnp.sum(keep, axis=0, keepdims=True).astype(jnp.float32)
        for piece in range(row_blocks // TILE):
            place = lane + piece * TILE
            until, before = none, none
            for other in range(pieces):
                until = until + jnp.where(rows_down[other] <= place, 1, 0)
                before = before + jnp.where(rows_down[other] < place, 1, 0)
            until = jnp.sum(until, axis=0, keepdims=True)
            before = jnp.sum(before, axis=0, keepdims=True)
            lasts[piece : piece + 1] = jnp.where(until == before, 0, until)
        moves = [
            pltpu.make_async_copy(source, target, order_sem.at[at])
            for at, (source, target) in enumerate(((words, meta_ref), (keeps, keep_ref), (lasts, last_ref)))
        ]
        for move in moves:
            move.start()
        for move in moves:
            move.wait()

    order()

    for piece in range(PIECES):
        tile_copy(piece).wait()

        def turn(step, carry):
            for offset in range(4):
                at = piece * (slots // PIECES) + step * 4 + offset
                tiles[at] = tiles[at].T
            return carry

        lax.fori_loop(0, slots // PIECES // 4, turn, 0)
        if piece == PIECES // 4:
            relay(0)
            if chunks > AHEAD:
                send_own(AHEAD)

    for w in kinds:
        by_kind[w][2][0] = jnp.zeros((w, TILE), jnp.float32)

    for p in range(phases):
        receive(p)
        if p + 1 < phases:
            relay(p + 1)
        if p + 1 + AHEAD < chunks:
            send_own(p + 1 + AHEAD)
        products(p)
        if p >= 2:
            settle(p - 2)
        finish(p)
        pair_sum(p)
        if p >= 1:
            chip_sum(p - 1)
    chip_sum(phases - 1)

    for p in (phases - 2, phases - 1):
        settle(p)
    for p in range(phases):
        sent(p)


def filter_bank(coefs, base_ref, first_ref, second_ref, out_ref):
    for at in range(0, base_ref.shape[1], TILE):
        lanes = slice(at, at + TILE)
        base = base_ref[:, lanes].astype(jnp.float32)
        first = first_ref[:, lanes].astype(jnp.float32)
        rest = 2.0 * second_ref[:, lanes].astype(jnp.float32) - base
        for scale, (zero, one, two) in enumerate(coefs):
            out_ref[scale, :, lanes] = (zero * base + one * first + two * rest).astype(out_ref.dtype)


def shards(features, tile_rows, tile_cols, tile_count, tile_data):
    row_size, col_size = lax.axis_size("row"), lax.axis_size("col")
    channels, nodes = features.shape
    slots = tile_rows.shape[2]
    slot_data = tile_data.reshape(slots, TILE, TILE)
    row_blocks = col_size * nodes // TILE
    slot_bits = (slots - 1).bit_length()
    col_bits = (row_size * nodes // TILE - 1).bit_length()
    phases = 2 * len(CHUNKS)
    chips = col_size // 2
    widths = [CHUNKS[p % len(CHUNKS)] for p in range(phases)]
    field = jax.ShapeDtypeStruct((channels, nodes), jnp.bfloat16)
    dma = pltpu.SemaphoreType.DMA
    per_block = nodes // TILE
    scratch = [VMEM((row_size * per_block, w, TILE), jnp.bfloat16) for w in widths]
    scratch += [VMEM((chips, per_block, w, TILE), jnp.bfloat16) for w in widths]
    scratch += [VMEM((chips - 1, per_block, w, TILE), jnp.bfloat16) for w in widths]
    for w in sorted(set(CHUNKS)):
        scratch += [VMEM((2, chips, per_block, w, TILE), jnp.bfloat16)] * 2
        scratch += [VMEM((slots + 1, w, TILE), jnp.float32)]
    scratch += [
        VMEM((slots, TILE, TILE), jnp.bfloat16),
        VMEM((channels, nodes), jnp.bfloat16),
        VMEM((slots // TILE, TILE), jnp.int32),
        VMEM((slots // TILE, TILE), jnp.float32),
        VMEM((row_blocks // TILE, TILE), jnp.int32),
        pltpu.SMEM((slots // TILE, TILE), jnp.int32),
        pltpu.SMEM((slots // TILE, TILE), jnp.float32),
        pltpu.SMEM((row_blocks // TILE, TILE), jnp.int32),
        dma((3,)),
        dma((len(CHUNKS),)),
        dma((PIECES,)),
        dma((phases, 2, 2 * row_size)),
        dma((phases, 2, row_size)),
        dma((phases, chips)),
        dma((phases, chips)),
        dma((phases, chips - 1)),
        dma((phases, chips - 1)),
    ]
    first, second = pl.pallas_call(
        functools.partial(body, (row_size, col_size, slots, slot_bits, col_bits)),
        out_shape=(field, field),
        in_specs=[
            pl.BlockSpec(memory_space=VMEM),
            pl.BlockSpec(memory_space=VMEM),
            pl.BlockSpec(memory_space=pltpu.SMEM),
            pl.BlockSpec(memory_space=pl.ANY),
            pl.BlockSpec(memory_space=pl.ANY),
        ],
        out_specs=(pl.BlockSpec(memory_space=VMEM), pl.BlockSpec(memory_space=VMEM)),
        scratch_shapes=scratch,
        compiler_params=pltpu.CompilerParams(
            collective_id=0, has_side_effects=True, vmem_limit_bytes=60 * 2**20
        ),
        name="operator_twice",
    )(tile_rows, tile_cols, tile_count, features, slot_data)

    depth = 32
    coefs = [tuple(float(c) for c in row) for row in zip(*coefficients())]
    rows = pl.BlockSpec((depth, nodes), lambda i: (i, 0))
    filtered = pl.pallas_call(
        functools.partial(filter_bank, coefs),
        out_shape=jax.ShapeDtypeStruct((SCALES, channels, nodes), jnp.bfloat16),
        grid=(channels // depth,),
        in_specs=[rows, rows, rows],
        out_specs=pl.BlockSpec((SCALES, depth, nodes), lambda i: (0, i, 0)),
        name="filter_bank",
    )(features, first, second)
    return filtered.reshape(SCALES * channels, nodes)


def solution(mesh):
    return jax.shard_map(
        shards,
        mesh=mesh,
        in_specs=(
            P(None, ("row", "col")),
            P("row", "col", None),
            P("row", "col", None),
            P("row", "col"),
            P("row", "col", None, None, None),
        ),
        out_specs=P(None, ("row", "col")),
        check_vma=False,
    )
```

```python
import functools

import jax
import jax.numpy as jnp
import numpy as np
from jax import lax
from jax.experimental import pallas as pl
from jax.experimental.pallas import tpu as pltpu
from jax.sharding import PartitionSpec as P

SCALES = 8
TILE = 128
MESH = pl.DeviceIdType.MESH
VMEM = pltpu.VMEM
CHUNKS = (16, 16, 16, 16)
UNROLL = TILE
PIECES = 8
REACH = 2
AHEAD = 4


def coefficients():
    times = np.float32(0.25) * np.float32(2.0) ** (np.arange(SCALES).astype(np.float32) / np.float32(2.0))
    halved = times / np.float32(2.0)
    square = halved * halved
    term_zero = np.ones_like(times)
    term_one = halved
    sum_zero, sum_one = term_zero, term_one
    for degree in range(1, 24):
        term_zero = term_zero * square / np.float32(degree * degree)
        term_one = term_one * square / np.float32(degree * (degree + 1))
        sum_zero = sum_zero + term_zero
        sum_one = sum_one + term_one
    damping = np.exp(-times)
    zero, one = damping * sum_zero, damping * sum_one
    return zero, np.float32(-2.0) * one, np.float32(2.0) * (zero - np.float32(2.0) * one / times)


def sign_of(way):
    return 1 - 2 * way


def body(plan, rows_ref, cols_ref, count_ref, features_ref, data_ref, first_ref, second_ref, *scratch):
    row_size, col_size, slots, slot_bits, col_bits = plan
    chunks = len(CHUNKS)
    phases = 2 * chunks
    names = list(scratch)
    panels = [names.pop(0) for _ in range(phases)]
    arrived_a = [names.pop(0) for _ in range(phases)]
    arrived_b = [names.pop(0) for _ in range(phases)]
    kinds = sorted(set(CHUNKS))
    by_kind = {w: (names.pop(0), names.pop(0), names.pop(0)) for w in kinds}
    first_held, second_held, out_sem, tiles, field, words, keeps, lasts, meta_ref, keep_ref, last_ref, order_sem, own_sem, tile_sem, zsend, zrecv, asend, arecv, bsend, brecv = names
    width = [CHUNKS[p % chunks] for p in range(phases)]
    start = [sum(CHUNKS[: p % chunks]) for p in range(phases)]
    partials = [by_kind[width[p]][p % 2] for p in range(phases)]
    sums = [by_kind[width[p]][2] for p in range(phases)]
    chips = col_size // 2
    per_block = first_ref.shape[1] // TILE
    row_blocks = col_size * per_block

    me = lax.axis_index("row")
    col = lax.axis_index("col")
    side = lax.rem(col, 2)
    chip = col // 2

    def own_copy(p):
        rows = pl.ds(start[p], width[p])
        return pltpu.make_async_copy(features_ref.at[rows], field.at[rows], own_sem.at[p])

    def tile_copy(piece):
        part = pl.ds(piece * (slots // PIECES), slots // PIECES)
        return pltpu.make_async_copy(data_ref.at[part], tiles.at[part], tile_sem.at[piece])

    for p in range(chunks):
        own_copy(p).start()
    for piece in range(PIECES):
        tile_copy(piece).start()

    barrier = pltpu.get_barrier_semaphore()
    expected = jnp.int32(0)
    for sign in (1, -1):
        for hop in range(1, min(REACH, row_size - 1) + 1):
            peer = me + sign * hop
            inside = jnp.logical_and(peer >= 0, peer < row_size)
            expected = expected + inside.astype(jnp.int32)

            @pl.when(inside)
            def _():
                pl.semaphore_signal(barrier, inc=1, device_id={"row": peer}, device_id_type=MESH)

    pl.semaphore_signal(barrier, inc=1, device_id={"col": col + 1 - 2 * side}, device_id_type=MESH)
    for step in range(1, chips):
        peer = 2 * lax.rem(chip + step, chips) + side
        pl.semaphore_signal(barrier, inc=1, device_id={"col": peer}, device_id_type=MESH)
    pl.semaphore_wait(barrier, expected + chips)

    def within(at):
        return jnp.logical_and(at >= 0, at < row_size)

    def last_of(way):
        return row_size - 1 if way == 0 else 0

    def zcopy(p, way, hop, origin, target, place=0):
        block = panels[p].at[pl.ds(origin * per_block, per_block)]
        return pltpu.make_async_remote_copy(
            src_ref=block,
            dst_ref=block,
            send_sem=zsend.at[p, way, place + hop - 1],
            recv_sem=zrecv.at[p, way, hop - 1],
            device_id={"row": target},
            device_id_type=MESH,
        )

    def direct(p, way, hop):
        target = me + sign_of(way) * hop
        inside = within(target)
        if hop > 1:
            inside = jnp.logical_and(inside, target != last_of(way))
        return inside, zcopy(p, way, hop, me, target)

    def relayed(p, way, hop):
        target = me + sign_of(way)
        origin = target - sign_of(way) * hop
        inside = jnp.logical_and(within(target), within(origin))
        if hop <= REACH:
            inside = jnp.logical_and(inside, target == last_of(way))
        return inside, zcopy(p, way, hop, origin, target, row_size)

    def landed(p, way, hop):
        origin = me - sign_of(way) * hop
        return within(origin), zcopy(p, way, hop, origin, origin)

    direct_hops = range(min(REACH, row_size - 1), 0, -1)
    relay_hops = range(2, row_size)

    def send_own(p):
        for hop in direct_hops:
            for way in range(2):
                inside, copy = direct(p, way, hop)
                pl.when(inside)(copy.start)

    def relay(p):
        for hop in relay_hops:
            for way in range(2):
                inside, copy = relayed(p, way, hop)
                arrival = landed(p, way, hop - 1)[1]

                @pl.when(inside)
                def _():
                    arrival.wait_recv()
                    copy.start()

    def receive(p):
        for hop in range(1, row_size):
            for way in range(2):
                inside, arrival = landed(p, way, hop)
                target = me + sign_of(way)
                passes = within(target)
                if hop + 1 <= REACH:
                    passes = jnp.logical_and(passes, target == last_of(way))
                inside = jnp.logical_and(inside, jnp.logical_not(passes))
                pl.when(inside)(arrival.wait_recv)

    def sent(p):
        for way in range(2):
            for hop in direct_hops:
                inside, copy = direct(p, way, hop)
                pl.when(inside)(copy.wait_send)
            for hop in relay_hops:
                inside, copy = relayed(p, way, hop)
                pl.when(inside)(copy.wait_send)

    def products(p):
        lanes_mask = (1 << col_bits) - 1
        channels = width[p]

        def group(index, total):
            left, right = [], []
            for offset in range(UNROLL):
                word = meta_ref[index, offset]
                column = jnp.bitwise_and(lax.shift_right_logical(word, slot_bits), lanes_mask)
                left.append(panels[p][column])
                right.append(tiles[jnp.bitwise_and(word, slots - 1)])
            parts = []
            for at in range(0, UNROLL, 2):
                both = jnp.dot(
                    jnp.concatenate(left[at : at + 2], 0),
                    jnp.concatenate(right[at : at + 2], 1),
                    preferred_element_type=jnp.float32,
                )
                parts += [both[:channels, :TILE], both[channels:, TILE:]]
            for offset in range(UNROLL):
                total = total * keep_ref[index, offset] + parts[offset]
                sums[p][1 + index * UNROLL + offset] = total
            return total

        empty = jnp.zeros((channels, TILE), jnp.float32)
        lax.fori_loop(0, slots // UNROLL, group, empty)

    def finish(p):
        def rows(target, side_of):
            dest = 2 * target + side_of
            line, first_at = dest * per_block // TILE, lax.rem(dest * per_block, TILE)
            for block in range(per_block):
                partials[p][side_of, target, block] = sums[p][
                    last_ref[line, first_at + block]
                ].astype(jnp.bfloat16)

        def given(step, carry):
            target = lax.rem(chip + step, chips)
            rows(target, 1 - side)
            acopy(p, target).start()
            return carry

        def kept(target, carry):
            rows(target, side)
            return carry

        lax.fori_loop(1, chips + 1, given, 0)
        lax.fori_loop(0, chips, kept, 0)

    def acopy(p, target):
        return pltpu.make_async_remote_copy(
            src_ref=partials[p].at[1 - side, target],
            dst_ref=arrived_a[p].at[target],
            send_sem=asend.at[p, target],
            recv_sem=arecv.at[p, target],
            device_id={"col": col + 1 - 2 * side},
            device_id_type=MESH,
        )

    def bcopy(p, step):
        target = lax.rem(chip + step, chips)
        return pltpu.make_async_remote_copy(
            src_ref=partials[p].at[side, target],
            dst_ref=arrived_b[p].at[step - 1],
            send_sem=bsend.at[p, step - 1],
            recv_sem=brecv.at[p, step - 1],
            device_id={"col": 2 * target + side},
            device_id_type=MESH,
        )

    def pair_sum(p):
        for step in [*range(1, chips), 0]:
            target = lax.rem(chip + step, chips)
            acopy(p, target).wait_recv()
            total = partials[p][side, target].astype(jnp.float32) + arrived_a[p][target].astype(jnp.float32)
            partials[p][side, target] = total.astype(jnp.bfloat16)
            if step:
                bcopy(p, step).start()

    def chip_sum(p):
        total = partials[p][side, chip].astype(jnp.float32)
        for step in range(1, chips):
            bcopy(p, step).wait_recv()
            total = total + arrived_b[p][step - 1].astype(jnp.float32)
        result = total.astype(jnp.bfloat16)
        if p < chunks:
            panels[p + chunks][pl.ds(me * per_block, per_block)] = result
            send_own(p + chunks)
        out_ref = first_held if p < chunks else second_held
        for block in range(per_block):
            out_ref[start[p] : start[p] + width[p], block * TILE : (block + 1) * TILE] = result[block]
        out_copy(p).start()

    def out_copy(p):
        rows = pl.ds(start[p], width[p])
        held, out = (first_held, first_ref) if p < chunks else (second_held, second_ref)
        return pltpu.make_async_copy(held.at[rows], out.at[rows], out_sem.at[p])

    def settle(p):
        for target in range(chips):
            acopy(p, target).wait_send()
        for step in range(1, chips):
            bcopy(p, step).wait_send()

    for p in range(chunks):
        own_copy(p).wait()
        for block in range(per_block):
            panels[p][me * per_block + block] = field[
                start[p] : start[p] + width[p], block * TILE : (block + 1) * TILE
            ]
        if p < AHEAD:
            send_own(p)

    def order():
        live = count_ref[0, 0]
        square = (TILE, TILE)
        lane = lax.broadcasted_iota(jnp.int32, square, 1)
        none = jnp.zeros(square, jnp.int32)
        keys, rows_lane, keys_down, rows_down, words_down = [], [], [], [], []
        pieces = slots // TILE
        for piece in range(pieces):
            part = slice(piece * TILE, (piece + 1) * TILE)
            index = lane + piece * TILE
            row = jnp.where(index < live, jnp.broadcast_to(rows_ref[0, :, part], square), row_blocks)
            word = index + jnp.broadcast_to(cols_ref[0, :, part], square) * slots
            keys.append(row * slots + index)
            rows_lane.append(row)
            keys_down.append(keys[-1].T)
            rows_down.append(row.T)
            words_down.append(word.T)
        ranks, repeats = [], []
        for piece in range(pieces):
            ahead, same = none, none
            for other in range(pieces):
                less = jnp.where(keys_down[other] < keys[piece], 1, 0)
                ahead = ahead + less
                same = same + jnp.where(rows_down[other] == rows_lane[piece], less, 0)
            ahead = jnp.sum(ahead, axis=0, keepdims=True)
            same = jnp.minimum(jnp.sum(same, axis=0, keepdims=True), 1)
            ranks.append(jnp.broadcast_to(ahead, square).T)
            repeats.append(jnp.broadcast_to(same, square).T)
        for piece in range(pieces):
            place = lane + piece * TILE
            word, keep = none, none
            for other in range(pieces):
                here = ranks[other] == place
                word = word + jnp.where(here, words_down[other], 0)
                keep = keep + jnp.where(here, repeats[other], 0)
            words[piece : piece + 1] = jnp.sum(word, axis=0, keepdims=True)
            keeps[piece : piece + 1] = jnp.sum(keep, axis=0, keepdims=True).astype(jnp.float32)
        for piece in range(row_blocks // TILE):
            place = lane + piece * TILE
            until, before = none, none
            for other in range(pieces):
                until = until + jnp.where(rows_down[other] <= place, 1, 0)
                before = before + jnp.where(rows_down[other] < place, 1, 0)
            until = jnp.sum(until, axis=0, keepdims=True)
            before = jnp.sum(before, axis=0, keepdims=True)
            lasts[piece : piece + 1] = jnp.where(until == before, 0, until)
        moves = [
            pltpu.make_async_copy(source, target, order_sem.at[at])
            for at, (source, target) in enumerate(((words, meta_ref), (keeps, keep_ref), (lasts, last_ref)))
        ]
        for move in moves:
            move.start()
        for move in moves:
            move.wait()

    order()

    for piece in range(PIECES):
        tile_copy(piece).wait()

        def turn(step, carry):
            for offset in range(4):
                at = piece * (slots // PIECES) + step * 4 + offset
                tiles[at] = tiles[at].T
            return carry

        lax.fori_loop(0, slots // PIECES // 4, turn, 0)
        if piece == PIECES // 4:
            relay(0)
            if chunks > AHEAD:
                send_own(AHEAD)

    for w in kinds:
        by_kind[w][2][0] = jnp.zeros((w, TILE), jnp.float32)

    for p in range(phases):
        receive(p)
        if p + 1 < phases:
            relay(p + 1)
        if p + 1 + AHEAD < chunks:
            send_own(p + 1 + AHEAD)
        products(p)
        if p >= 2:
            settle(p - 2)
        finish(p)
        pair_sum(p)
        if p >= 1:
            chip_sum(p - 1)
    chip_sum(phases - 1)

    for p in (phases - 2, phases - 1):
        settle(p)
    for p in range(phases):
        sent(p)
        out_copy(p).wait()


def filter_bank(coefs, base_ref, first_ref, second_ref, out_ref):
    for at in range(0, base_ref.shape[1], TILE):
        lanes = slice(at, at + TILE)
        base = base_ref[:, lanes].astype(jnp.float32)
        first = first_ref[:, lanes].astype(jnp.float32)
        rest = 2.0 * second_ref[:, lanes].astype(jnp.float32) - base
        for scale, (zero, one, two) in enumerate(coefs):
            out_ref[scale, :, lanes] = (zero * base + one * first + two * rest).astype(out_ref.dtype)


def shards(features, tile_rows, tile_cols, tile_count, tile_data):
    row_size, col_size = lax.axis_size("row"), lax.axis_size("col")
    channels, nodes = features.shape
    slots = tile_rows.shape[2]
    slot_data = tile_data.reshape(slots, TILE, TILE)
    row_blocks = col_size * nodes // TILE
    slot_bits = (slots - 1).bit_length()
    col_bits = (row_size * nodes // TILE - 1).bit_length()
    phases = 2 * len(CHUNKS)
    chips = col_size // 2
    widths = [CHUNKS[p % len(CHUNKS)] for p in range(phases)]
    field = jax.ShapeDtypeStruct((channels, nodes), jnp.bfloat16)
    dma = pltpu.SemaphoreType.DMA
    per_block = nodes // TILE
    scratch = [VMEM((row_size * per_block, w, TILE), jnp.bfloat16) for w in widths]
    scratch += [VMEM((chips, per_block, w, TILE), jnp.bfloat16) for w in widths]
    scratch += [VMEM((chips - 1, per_block, w, TILE), jnp.bfloat16) for w in widths]
    for w in sorted(set(CHUNKS)):
        scratch += [VMEM((2, chips, per_block, w, TILE), jnp.bfloat16)] * 2
        scratch += [VMEM((slots + 1, w, TILE), jnp.float32)]
    scratch += [
        VMEM((channels, nodes), jnp.bfloat16),
        VMEM((channels, nodes), jnp.bfloat16),
        dma((phases,)),
        VMEM((slots, TILE, TILE), jnp.bfloat16),
        VMEM((channels, nodes), jnp.bfloat16),
        VMEM((slots // TILE, TILE), jnp.int32),
        VMEM((slots // TILE, TILE), jnp.float32),
        VMEM((row_blocks // TILE, TILE), jnp.int32),
        pltpu.SMEM((slots // TILE, TILE), jnp.int32),
        pltpu.SMEM((slots // TILE, TILE), jnp.float32),
        pltpu.SMEM((row_blocks // TILE, TILE), jnp.int32),
        dma((3,)),
        dma((len(CHUNKS),)),
        dma((PIECES,)),
        dma((phases, 2, 2 * row_size)),
        dma((phases, 2, row_size)),
        dma((phases, chips)),
        dma((phases, chips)),
        dma((phases, chips - 1)),
        dma((phases, chips - 1)),
    ]
    first, second = pl.pallas_call(
        functools.partial(body, (row_size, col_size, slots, slot_bits, col_bits)),
        out_shape=(field, field),
        in_specs=[
            pl.BlockSpec(memory_space=VMEM),
            pl.BlockSpec(memory_space=VMEM),
            pl.BlockSpec(memory_space=pltpu.SMEM),
            pl.BlockSpec(memory_space=pl.ANY),
            pl.BlockSpec(memory_space=pl.ANY),
        ],
        out_specs=(pl.BlockSpec(memory_space=pl.ANY), pl.BlockSpec(memory_space=pl.ANY)),
        scratch_shapes=scratch,
        compiler_params=pltpu.CompilerParams(
            collective_id=0, has_side_effects=True, vmem_limit_bytes=60 * 2**20
        ),
        name="operator_twice",
    )(tile_rows, tile_cols, tile_count, features, slot_data)

    depth = 32
    coefs = [tuple(float(c) for c in row) for row in zip(*coefficients())]
    rows = pl.BlockSpec((depth, nodes), lambda i: (i, 0))
    filtered = pl.pallas_call(
        functools.partial(filter_bank, coefs),
        out_shape=jax.ShapeDtypeStruct((SCALES, channels, nodes), jnp.bfloat16),
        grid=(channels // depth,),
        in_specs=[rows, rows, rows],
        out_specs=pl.BlockSpec((SCALES, depth, nodes), lambda i: (0, i, 0)),
        name="filter_bank",
    )(features, first, second)
    return filtered.reshape(SCALES * channels, nodes)


def solution(mesh):
    return jax.shard_map(
        shards,
        mesh=mesh,
        in_specs=(
            P(None, ("row", "col")),
            P("row", "col", None),
            P("row", "col", None),
            P("row", "col"),
            P("row", "col", None, None, None),
        ),
        out_specs=P(None, ("row", "col")),
        check_vma=False,
    )
```
